32 devices in a mesh: bank: 4 (over x, core), zero: 8 (over z, y).
Axes of the slice: x: 2, y: 2, z: 4, core: 2. Of those that a mesh axis runs over, the one named last changes fastest.
Arguments:
- w_gate: float32 [64, 2048, 1024], P('bank', 'zero'), may hold values from -0.1875 to 0.1875
- avg_gate: float32 [64, 2048, 1024], P('bank', 'zero'), may hold values from -0.125 to 0.125
- w_up: float32 [64, 2048, 1024], P('bank', 'zero'), may hold values from -0.1875 to 0.1875
- avg_up: float32 [64, 2048, 1024], P('bank', 'zero'), may hold values from -0.125 to 0.125
- mix_share: float32 [64], P('bank'), may hold values from 0.2 to 0.8
- router_weight: float32 [2048, 64], P('zero', 'bank'), may hold values from -0.125 to 0.125
- router_gain: float32 [2048], P('zero'), may hold values from 0.25 to 1.75
Outputs:
- serve_gate: bfloat16 [64, 2048, 1024], P('bank', None, 'zero')
- serve_up: bfloat16 [64, 2048, 1024], P('bank', None, 'zero')
- scale_gate: float32 [64, 1024], P('bank', 'zero')
- scale_up: float32 [64, 1024], P('bank', 'zero')
- serve_router: bfloat16 [2048, 64], replicated
The draws below stay inside these ranges and needn't reach their ends.
All inputs are finite; a program needn't handle non-finite values. Where the reference program divides by a largest or mean magnitude, that divisor is 1e-20 or more.
Results may differ from the reference program's by a relative error of at most 0.001.
Values may be sent and summed in bfloat16 or wider, within the bound.
No kernel may reach another device: no remote copies, remote signals or barrier semaphores. Data moves between devices by JAX's collectives and lax.ppermute only.
A program may use at most 256 MiB of HBM per device.

```python
import jax
import jax.numpy as jnp

EXPERTS = 64
D_MODEL = 2048
D_EXPERT = 1024


def strengthened(drawn, key, source, target, parts, factor):
    def block_of(position):
        return (jnp.arange(drawn.shape[position]) // (drawn.shape[position] // parts)).reshape((-1,) + (1,) * (drawn.ndim - 1 - position))

    near = jax.random.permutation(key, parts)[block_of(target)]
    second = (block_of(target) + parts // 2) % parts
    return jnp.where((block_of(source) == near) | (block_of(source) == second), factor * drawn, drawn)


def levels(rng, dims, shards, smallest, largest):
    def one(axis_at, blocks):
        steps = jax.random.uniform(jax.random.fold_in(jax.random.fold_in(rng, 6), axis_at), (blocks,), jnp.float32, smallest / len(shards), largest / len(shards))
        return jnp.repeat(jnp.exp(steps), dims[axis_at] // blocks).reshape((-1,) + (1,) * (len(dims) - axis_at - 1))

    factor_of = one(*shards[0])
    for cut in shards[1:]:
        factor_of = factor_of * one(*cut)
    return factor_of


def gaussian(key, dims, deviation, most, pieces=(), kind=jnp.bfloat16):
    array = jax.random.normal(key, dims, jnp.float32) * deviation
    if len(pieces) > 0:
        array = levels(key, dims, pieces, -0.22, 0.18) * array
    return jnp.clip(array, min=-most, max=most).astype(kind)


def heavy_noise(stream_key, extent, scale, bound, pieces, heavy, held_as=jnp.bfloat16):
    array = scale * jax.random.normal(stream_key, extent, jnp.float32)
    if pieces:
        array = array * levels(stream_key, extent, pieces, -0.22, 0.18)
    return jnp.clip(strengthened(array, jax.random.fold_in(stream_key, 3), *heavy), -bound, bound).astype(held_as)


def setup_inputs(seed: int = 0) -> dict:
    arg_keys = jax.random.split(jax.random.key(seed), 8)
    w_gate = heavy_noise(arg_keys[0], (EXPERTS, D_MODEL, D_EXPERT), D_MODEL ** -0.5, 0.1875, ((0, 4), (1, 8)), (1, 2, 8, 2.0), jnp.float32)
    avg_gate = gaussian(arg_keys[1], (EXPERTS, D_MODEL, D_EXPERT), D_MODEL ** -0.5, 0.125, ((0, 4), (1, 8)), jnp.float32)
    w_up = heavy_noise(arg_keys[2], (EXPERTS, D_MODEL, D_EXPERT), D_MODEL ** -0.5, 0.1875, ((0, 4), (1, 8)), (1, 2, 8, 2.0), jnp.float32)
    avg_up = gaussian(arg_keys[3], (EXPERTS, D_MODEL, D_EXPERT), D_MODEL ** -0.5, 0.125, ((0, 4), (1, 8)), jnp.float32)
    mix_share = jnp.clip(0.2 + 0.6 * jax.random.uniform(arg_keys[4], (EXPERTS,), jnp.float32) ** levels(arg_keys[4], (EXPERTS,), ((0, 4),), -0.2, 0.2), 0.2, 0.8)
    router_weight = gaussian(arg_keys[5], (D_MODEL, EXPERTS), D_MODEL ** -0.5, 0.125, ((0, 8), (1, 4)), jnp.float32)
    router_gain = jnp.clip(1.0 + 0.15 * jax.random.normal(arg_keys[6], (D_MODEL,), jnp.float32), 0.25, 1.75)
    return {"w_gate": w_gate, "avg_gate": avg_gate, "w_up": w_up, "avg_up": avg_up, "mix_share": mix_share, "router_weight": router_weight, "router_gain": router_gain}


def reference(w_gate, avg_gate, w_up, avg_up, mix_share, router_weight, router_gain):
    fresh_gate = mix_share[:, None, None] * w_gate + (1.0 - mix_share[:, None, None]) * avg_gate
    fresh_up = mix_share[:, None, None] * w_up + (1.0 - mix_share[:, None, None]) * avg_up
    scale_gate = jnp.sum(jnp.abs(fresh_gate), axis=1) / D_MODEL
    serve_gate = (fresh_gate / jnp.expand_dims(scale_gate, 1)).astype(jnp.bfloat16)
    scale_up = jnp.sum(jnp.abs(fresh_up), axis=1) / D_MODEL
    serve_up = (fresh_up / jnp.expand_dims(scale_up, 1)).astype(jnp.bfloat16)
    serve_router = (router_weight * router_gain[:, None]).astype(jnp.bfloat16)
    return serve_gate, serve_up, scale_gate, scale_up, serve_router
```

```python
import functools

import jax
import jax.numpy as jnp
from jax import lax
from jax.experimental import pallas as pl
from jax.experimental.pallas import tpu as pltpu
from jax.sharding import PartitionSpec as P


GATE_GROUPS = ((4, 2), (5, 5))
UP_GROUPS = ((5, 5, 4, 2),)

DEPTH = 3

SMEM = pl.BlockSpec(memory_space=pltpu.SMEM)
ANY = pl.BlockSpec(memory_space=pl.ANY)
TOKEN = (8, 128)


def spans(groups, experts):
    whole = sum(map(sum, groups))
    at, out = 0, []
    for group in groups:
        chunks = []
        for share in group:
            first, last = at * experts // whole, (at + share) * experts // whole
            at += share
            if last > first:
                chunks.append((first, last - first))
        if chunks:
            out.append(chunks)
    return out


def sums_body(first, step, mix_ref, w_ref, avg_ref, *refs):
    out_ref = refs[-1]
    for i in range(step):
        at = pl.program_id(0) * step + i
        mix = mix_ref[first + at]
        fresh = mix * w_ref[i] + (1.0 - mix) * avg_ref[i]
        out_ref[pl.ds(at, 1), :] = jnp.sum(jnp.abs(fresh), axis=0, keepdims=True)


def sums(mix, w, avg, first, count, after):
    _, rows, cols = w.shape
    step = next(s for s in (4, 2, 1) if count % s == 0 and first % s == 0)
    block = pl.BlockSpec((step, rows, cols), lambda e: (first // step + e, 0, 0))
    return pl.pallas_call(
        functools.partial(sums_body, first, step),
        grid=(count // step,),
        in_specs=[SMEM, block, block] + [ANY] * len(after),
        out_specs=pl.BlockSpec((count, cols), lambda e: (0, 0)),
        out_shape=jax.ShapeDtypeStruct((count, cols), jnp.float32),
        name="sums",
    )(mix, w, avg, *after)


def pack_body(first, skip, ways, me_ref, mix_ref, w_ref, avg_ref, total_ref, *refs):
    out_refs, held_ref = refs[-1 - ways : -1], refs[-1]
    me = me_ref[0]
    at = pl.program_id(0)
    mix = mix_ref[first + at]
    rows = w_ref.shape[1]
    width = w_ref.shape[2] // ways
    inverse = 1.0 / (total_ref[pl.ds(skip + at, 1), :] * (1.0 / (ways * rows)))
    for j in range(ways):
        cut = slice(j * width, (j + 1) * width)
        fresh = mix * w_ref[0, :, cut] + (1.0 - mix) * avg_ref[0, :, cut]
        held_ref[me ^ j] = (fresh * inverse[:, cut]).astype(jnp.bfloat16)
    for k in range(ways):
        out_refs[k][0] = held_ref[k]


def pack(me, mix, w, avg, total, first, count, skip, ways, after):
    _, rows, cols = w.shape
    block = pl.BlockSpec((1, rows, cols), lambda e: (first + e, 0, 0))
    piece = (rows, cols // ways)
    return pl.pallas_call(
        functools.partial(pack_body, first, skip, ways),
        grid=(count,),
        in_specs=[SMEM, SMEM, block, block, pl.BlockSpec(total.shape, lambda e: (0, 0))]
        + [ANY] * len(after),
        out_specs=[pl.BlockSpec((1,) + piece, lambda e: (e, 0, 0))] * ways,
        out_shape=[jax.ShapeDtypeStruct((count,) + piece, jnp.bfloat16)] * ways,
        scratch_shapes=[pltpu.VMEM((ways,) + piece, jnp.bfloat16)],
        name="pack",
    )(me, mix, w, avg, total, *after)


def unpack_body(ways, me_ref, *refs):
    out_ref, token_ref = refs[-2:]
    me = me_ref[0]
    rows = refs[0].shape[1]
    for k in range(ways):
        at = pl.multiple_of((me ^ k) * rows, rows)
        out_ref[0, pl.ds(at, rows), :] = refs[k][0]
    token_ref[...] = jnp.zeros(token_ref.shape, token_ref.dtype)


def unpack(me, received, whole, first, total, after=()):
    ways = len(received)
    count, rows, width = received[0].shape
    held = [] if whole is None else [whole]
    return pl.pallas_call(
        functools.partial(unpack_body, ways),
        grid=(count,),
        in_specs=[SMEM]
        + [pl.BlockSpec((1, rows, width), lambda e: (e, 0, 0))] * ways
        + [ANY] * (len(held) + len(after)),
        out_specs=[
            pl.BlockSpec((1, ways * rows, width), lambda e: (first + e, 0, 0)),
            pl.BlockSpec(TOKEN, lambda e: (0, 0)),
        ],
        out_shape=[
            jax.ShapeDtypeStruct((total, ways * rows, width), jnp.bfloat16),
            jax.ShapeDtypeStruct(TOKEN, jnp.float32),
        ],
        input_output_aliases={1 + ways: 0} if held else {},
        name="unpack",
    )(me, *received, *held, *after)


def swap(value, k, axis, ways):
    return lax.ppermute(value, axis, [(d, d ^ k) for d in range(ways)])


def router_fold_body(weight_ref, gain_ref, *refs):
    refs[-1][...] = (weight_ref[...] * gain_ref[...]).astype(jnp.bfloat16)


def router_fold(weight, gain, after):
    full = lambda shape: pl.BlockSpec(shape, lambda: (0, 0))
    return pl.pallas_call(
        router_fold_body,
        in_specs=[full(weight.shape), full(gain.shape)] + [ANY] * len(after),
        out_specs=full(weight.shape),
        out_shape=jax.ShapeDtypeStruct(weight.shape, jnp.bfloat16),
        name="router_fold",
    )(weight, gain, *after)


def join_body(ways, axis, me_ref, *refs):
    out_ref = refs[-1]
    size = refs[0].shape[axis]
    for k in range(ways):
        if out_ref.ndim == 3:
            out_ref[me_ref[0] ^ k] = refs[k][...]
            continue
        at = pl.ds(pl.multiple_of((me_ref[0] ^ k) * size, size), size)
        if axis == 0:
            out_ref[at, :] = refs[k][...]
        else:
            out_ref[:, at] = refs[k][...]


def join(me, pieces, axis):
    ways = len(pieces)
    piece = pieces[0].shape
    shape = list(piece)
    shape[axis] *= ways
    aligned = axis == 0 or piece[axis] % 128 == 0
    made = tuple(shape) if aligned else (ways,) + piece
    out = pl.pallas_call(
        functools.partial(join_body, ways, axis),
        in_specs=[SMEM] + [pl.BlockSpec(piece, lambda: (0, 0))] * ways,
        out_specs=pl.BlockSpec(made, lambda: (0,) * len(made)),
        out_shape=jax.ShapeDtypeStruct(made, jnp.bfloat16),
        name="join",
    )(me, *pieces)
    return out if aligned else jnp.swapaxes(out, 0, 1).reshape(shape)


def doubling(partial, ways):
    stages = [partial]
    k = 1
    while k < ways:
        stages.append(stages[-1] + swap(stages[-1], k, "zero", ways))
        k *= 2
    return stages


def on_device(ways, banks, w_gate, avg_gate, w_up, avg_up, mix_share, router_weight, router_gain):
    experts, rows, cols = w_gate.shape
    width = cols // ways
    index = lax.axis_index("zero")
    me = jnp.reshape(index, (1,))
    my_bank = jnp.reshape(lax.axis_index("bank"), (1,))

    groups = [(0, chunks) for chunks in spans(GATE_GROUPS, experts)]
    groups += [(1, chunks) for chunks in spans(UP_GROUPS, experts)]
    pairs = ((w_gate, avg_gate), (w_up, avg_up))

    def group_stages(g, after):
        which, chunks = groups[g]
        count = sum(n for _, n in chunks)
        return doubling(sums(mix_share, *pairs[which], chunks[0][0], count, after), ways)

    served = [None, None]
    totals = [[], []]
    tokens = []
    pending = []

    def land(after=()):
        which, first, received = pending.pop(0)
        served[which], token = unpack(me, received, served[which], first, experts, after)
        tokens.append(token)

    router = None
    joined = None
    stages = group_stages(0, [])
    ahead = None
    for g, (which, chunks) in enumerate(groups):
        total = stages[-1]
        totals[which].append(total)
        stages = None
        for c, (first, count) in enumerate(chunks):
            after = []
            if len(pending) == DEPTH:
                land()
                after.append(tokens[-1])
            if stages is not None and c == 1:
                after.append(stages[-2])
            skip = first - chunks[0][0]
            sent = pack(me, mix_share, *pairs[which], total, first, count, skip, ways, after)
            received = [sent[0]] + [None] * (ways - 1)
            for k in reversed(range(1, ways)):
                received[k] = swap(sent[k], k, "zero", ways)
            pending.append((which, first, received))
            if c == 0 and g + 1 < len(groups):
                stages = group_stages(g + 1, [sent[0] if ahead is None else ahead])
            if router is None and tokens:
                router = router_fold(router_weight.T, router_gain[None, :], [tokens[-1]])
                columns = [router] + [swap(router, k, "bank", banks) for k in range(1, banks)]
                columns = join(my_bank, columns, 0)
                columns = [columns] + [swap(columns, k, "zero", ways) for k in range(1, ways)]
                joined = join(me, columns, 1)
        ahead = sent[0]
    while pending:
        land([joined] if len(pending) == 1 else [])

    scales = []
    for parts in totals:
        own = [lax.dynamic_slice_in_dim(t, index * width, width, axis=1) for t in parts]
        scales.append(jnp.concatenate(own, axis=0) / (ways * rows))
    return (served[0], served[1], scales[0], scales[1], joined.T)


def solution(mesh):
    ways, banks = mesh.shape["zero"], mesh.shape["bank"]
    assert ways & (ways - 1) == 0 and banks & (banks - 1) == 0
    in_specs = (
        P("bank", "zero", None),
        P("bank", "zero", None),
        P("bank", "zero", None),
        P("bank", "zero", None),
        P("bank"),
        P("zero", "bank"),
        P("zero"),
    )
    out_specs = (
        P("bank", None, "zero"),
        P("bank", None, "zero"),
        P("bank", "zero"),
        P("bank", "zero"),
        P(),
    )
    return jax.shard_map(
        functools.partial(on_device, ways, banks),
        mesh=mesh,
        in_specs=in_specs,
        out_specs=out_specs,
        check_vma=False,
    )
```

```python
import functools

import jax
import jax.numpy as jnp
from jax import lax
from jax.experimental import pallas as pl
from jax.experimental.pallas import tpu as pltpu
from jax.sharding import PartitionSpec as P


GATE_GROUPS = ((4, 4), (4, 4))
UP_GROUPS = ((6, 6, 3, 1),)

SMEM = pl.BlockSpec(memory_space=pltpu.SMEM)
ANY = pl.BlockSpec(memory_space=pl.ANY)


def spans(groups, experts):
    whole = sum(map(sum, groups))
    at, out = 0, []
    for group in groups:
        chunks = []
        for share in group:
            first, last = at * experts // whole, (at + share) * experts // whole
            at += share
            if last > first:
                chunks.append((first, last - first))
        if chunks:
            out.append(chunks)
    return out


def step_of(most, *counts):
    return next(n for n in range(most, 0, -1) if all(count % n == 0 for count in counts))


def sums_body(first, step, mix_ref, w_ref, avg_ref, *refs):
    out_ref = refs[-1]
    for i in range(step):
        at = pl.program_id(0) * step + i
        mix = mix_ref[first + at]
        fresh = mix * w_ref[i] + (1.0 - mix) * avg_ref[i]
        out_ref[pl.ds(at, 1), :] = jnp.sum(jnp.abs(fresh), axis=0, keepdims=True)


def sums(mix, w, avg, first, count):
    _, rows, cols = w.shape
    step = step_of(4 if first else 2, count, first)
    block = pl.BlockSpec((step, rows, cols), lambda e: (first // step + e, 0, 0))
    return pl.pallas_call(
        functools.partial(sums_body, first, step),
        grid=(count // step,),
        in_specs=[SMEM, block, block],
        out_specs=pl.BlockSpec((count, cols), lambda e: (0, 0)),
        out_shape=jax.ShapeDtypeStruct((count, cols), jnp.float32),
        name="sums",
    )(mix, w, avg)


def pack_body(first, skip, ways, me_ref, mix_ref, w_ref, avg_ref, *refs):
    addends, out_refs, held_ref = refs[: -1 - ways], refs[-1 - ways : -1], refs[-1]
    me = me_ref[0]
    step, rows, cols = w_ref.shape
    width = cols // ways
    for i in range(step):
        at = pl.program_id(0) * step + i
        mix = mix_ref[first + at]
        row = pl.ds(skip + at, 1)
        total = sum(ref[row, :] for ref in addends)
        inverse = 1.0 / (total * (1.0 / (ways * rows)))
        for j in range(ways):
            cut = slice(j * width, (j + 1) * width)
            fresh = mix * w_ref[i, :, cut] + (1.0 - mix) * avg_ref[i, :, cut]
            held_ref[me ^ j] = (fresh * inverse[:, cut]).astype(jnp.bfloat16)
        for k in range(ways):
            out_refs[k][i] = held_ref[k]


def pack(me, mix, w, avg, addends, first, count, skip, ways):
    _, rows, cols = w.shape
    step = step_of(2, count, first)
    block = pl.BlockSpec((step, rows, cols), lambda e: (first // step + e, 0, 0))
    piece = (rows, cols // ways)
    return pl.pallas_call(
        functools.partial(pack_body, first, skip, ways),
        grid=(count // step,),
        in_specs=[SMEM, SMEM, block, block]
        + [pl.BlockSpec(addends[0].shape, lambda e: (0, 0))] * len(addends),
        out_specs=[pl.BlockSpec((step,) + piece, lambda e: (e, 0, 0))] * ways,
        out_shape=[jax.ShapeDtypeStruct((count,) + piece, jnp.bfloat16)] * ways,
        scratch_shapes=[pltpu.VMEM((ways,) + piece, jnp.bfloat16)],
        name="pack",
    )(me, mix, w, avg, *addends)


def unpack_body(ways, me_ref, *refs):
    out_ref = refs[-1]
    me = me_ref[0]
    step, rows, _ = refs[0].shape
    for k in range(ways):
        at = pl.multiple_of((me ^ k) * rows, rows)
        for i in range(step):
            out_ref[i, pl.ds(at, rows), :] = refs[k][i]


def unpack(me, received, whole, first, total):
    ways = len(received)
    count, rows, width = received[0].shape
    step = step_of(4, count, first)
    held = [] if whole is None else [whole]
    return pl.pallas_call(
        functools.partial(unpack_body, ways),
        grid=(count // step,),
        in_specs=[SMEM]
        + [pl.BlockSpec((step, rows, width), lambda e: (e, 0, 0))] * ways
        + [ANY] * len(held),
        out_specs=pl.BlockSpec((step, ways * rows, width), lambda e: (first // step + e, 0, 0)),
        out_shape=jax.ShapeDtypeStruct((total, ways * rows, width), jnp.bfloat16),
        input_output_aliases={1 + ways: 0} if held else {},
        name="unpack",
    )(me, *received, *held)


def swap(value, k, axis, ways):
    return lax.ppermute(value, axis, [(d, d ^ k) for d in range(ways)])


def crossings(ways):
    return list(reversed(range(1, ways)))


def doublings(ways):
    return [1 << b for b in range(ways.bit_length() - 1)]


def router_fold_body(weight_ref, gain_ref, out_ref):
    out_ref[...] = (weight_ref[...] * gain_ref[...]).astype(jnp.bfloat16)


def router_fold(weight, gain):
    full = lambda shape: pl.BlockSpec(shape, lambda: (0, 0))
    return pl.pallas_call(
        router_fold_body,
        in_specs=[full(weight.shape), full(gain.shape)],
        out_specs=full(weight.shape),
        out_shape=jax.ShapeDtypeStruct(weight.shape, jnp.bfloat16),
        name="router_fold",
    )(weight, gain)


def join_body(places, axis, me_ref, in_ref, out_ref):
    size = in_ref.shape[1 + axis]
    for i, place in enumerate(places):
        at = me_ref[0] ^ place
        if out_ref.ndim == 3:
            out_ref[at] = in_ref[i]
        elif axis == 0:
            out_ref[pl.ds(pl.multiple_of(at * size, size), size), :] = in_ref[i]
        else:
            out_ref[:, pl.ds(pl.multiple_of(at * size, size), size)] = in_ref[i]


def join(me, pieces, places, axis):
    shape = list(pieces.shape[1:])
    aligned = axis == 0 or shape[axis] % 128 == 0
    shape[axis] *= len(places)
    made = tuple(shape) if aligned else pieces.shape
    out = pl.pallas_call(
        functools.partial(join_body, places, axis),
        in_specs=[SMEM, pl.BlockSpec(pieces.shape, lambda: (0, 0, 0))],
        out_specs=pl.BlockSpec(made, lambda: (0,) * len(made)),
        out_shape=jax.ShapeDtypeStruct(made, jnp.bfloat16),
        name="join",
    )(me, pieces)
    return out if aligned else jnp.swapaxes(out, 0, 1).reshape(shape)


def gather(value, me, axis, ways, along):
    pieces, places = value[None], [0]
    for k in reversed(doublings(ways)):
        pieces = jnp.concatenate([pieces, swap(pieces, k, axis, ways)], axis=0)
        places = places + [place ^ k for place in places]
    return join(me, pieces, places, along)


def on_device(ways, banks, w_gate, avg_gate, w_up, avg_up, mix_share, router_weight, router_gain):
    experts, rows, cols = w_gate.shape
    width = cols // ways
    index = lax.axis_index("zero")
    me = jnp.reshape(index, (1,))
    my_bank = jnp.reshape(lax.axis_index("bank"), (1,))

    served, scales = [], []
    g = c = 0
    for w, avg, shares in ((w_gate, avg_gate, GATE_GROUPS), (w_up, avg_up, UP_GROUPS)):
        whole, own = None, []
        for chunks in spans(shares, experts):
            start = chunks[0][0]
            total = sums(mix_share, w, avg, start, sum(n for _, n in chunks))
            for k in doublings(ways):
                addends = [total, swap(total, k, "zero", ways)]
                total = addends[0] + addends[1]
            own.append(lax.dynamic_slice_in_dim(total, index * width, width, axis=1))
            for first, count in chunks:
                sent = pack(me, mix_share, w, avg, addends, first, count, first - start, ways)
                received = list(sent)
                for k in crossings(ways):
                    received[k] = swap(sent[k], k, "zero", ways)
                whole = unpack(me, received, whole, first, experts)
                c += 1
            g += 1
        served.append(whole)
        scales.append(jnp.concatenate(own, axis=0) / (ways * rows))

    router = router_fold(router_weight.T, router_gain[None, :])
    router = gather(router, me, "zero", ways, 1)
    router = gather(router, my_bank, "bank", banks, 0)
    return (served[0], served[1], scales[0], scales[1], router.T)


def solution(mesh):
    ways, banks = mesh.shape["zero"], mesh.shape["bank"]
    assert ways & (ways - 1) == 0 and banks & (banks - 1) == 0
    in_specs = (
        P("bank", "zero", None),
        P("bank", "zero", None),
        P("bank", "zero", None),
        P("bank", "zero", None),
        P("bank"),
        P("zero", "bank"),
        P("zero"),
    )
    out_specs = (
        P("bank", None, "zero"),
        P("bank", None, "zero"),
        P("bank", "zero"),
        P("bank", "zero"),
        P(),
    )

    def step(*args):
        def body(*local):
            return on_device(ways, banks, *local)

        local = jax.shard_map(
            body, mesh=mesh, in_specs=in_specs, out_specs=out_specs, check_vma=False
        )
        return local(*args)

    return step
```

```python
import functools

import jax
import jax.numpy as jnp
from jax import lax
from jax.experimental import pallas as pl
from jax.experimental.pallas import tpu as pltpu
from jax.sharding import PartitionSpec as P


GATE_GROUPS = ((4, 4), (4, 4))
UP_GROUPS = ((6, 6, 3, 1),)

HALVED = 1

SMEM = pl.BlockSpec(memory_space=pltpu.SMEM)
ANY = pl.BlockSpec(memory_space=pl.ANY)
SUBLANES = 8


def spans(groups, experts):
    whole = sum(map(sum, groups))
    at, out = 0, []
    for group in groups:
        chunks = []
        for share in group:
            first, last = at * experts // whole, (at + share) * experts // whole
            at += share
            if last > first:
                chunks.append((first, last - first))
        if chunks:
            out.append(chunks)
    return out


def step_of(most, *counts):
    return next(n for n in range(most, 0, -1) if all(count % n == 0 for count in counts))


def sum_of(mix, w_ref, avg_ref, i):
    held = None
    for r in range(0, w_ref.shape[1], SUBLANES):
        cut = slice(r, r + SUBLANES)
        size = jnp.abs(mix * w_ref[i, cut, :] + (1.0 - mix) * avg_ref[i, cut, :])
        held = size if held is None else held + size
    return jnp.sum(held, axis=0, keepdims=True)


def sums_body(first, step, mix_ref, w_ref, avg_ref, out_ref):
    for i in range(step):
        at = pl.program_id(0) * step + i
        out_ref[pl.ds(at, 1), :] = sum_of(mix_ref[first + at], w_ref, avg_ref, i)


def sums(mix, w, avg, first, count):
    _, rows, cols = w.shape
    step = step_of(4, count, first)
    block = pl.BlockSpec((step, rows, cols), lambda e: (first // step + e, 0, 0))
    return pl.pallas_call(
        functools.partial(sums_body, first, step),
        grid=(count // step,),
        in_specs=[SMEM, block, block],
        out_specs=pl.BlockSpec((count, cols), lambda e: (0, 0)),
        out_shape=jax.ShapeDtypeStruct((count, cols), jnp.float32),
        name="sums",
    )(mix, w, avg)


def pack_body(first, skip, ways, pieces, me_ref, mix_ref, w_ref, avg_ref, *refs):
    addends, out_refs, held_ref = refs[: -1 - pieces], refs[-1 - pieces : -1], refs[-1]
    low = me_ref[0] & (pieces - 1)
    step, rows, cols = w_ref.shape
    width = cols // pieces
    for i in range(step):
        at = pl.program_id(0) * step + i
        mix = mix_ref[first + at]
        row = pl.ds(skip + at, 1)
        total = sum(ref[row, :] for ref in addends)
        inverse = 1.0 / (total * (1.0 / (ways * rows)))
        for j in range(pieces):
            cut = slice(j * width, (j + 1) * width)
            fresh = mix * w_ref[i, :, cut] + (1.0 - mix) * avg_ref[i, :, cut]
            held_ref[low ^ j] = (fresh * inverse[:, cut]).astype(jnp.bfloat16)
        for k in range(pieces):
            out_refs[k][i] = held_ref[k]


def pack(me, mix, w, avg, addends, first, count, skip, ways, part=None):
    _, rows, cols = w.shape
    step = step_of(2, count, first)
    pieces = ways if part is None else ways // 2

    def side(me_ref):
        if part is None:
            return 0
        return (me_ref[0] >> (pieces.bit_length() - 1)) ^ part

    block = pl.BlockSpec(
        (step, rows, cols * pieces // ways), lambda e, me_ref: (first // step + e, 0, side(me_ref))
    )
    sums_block = pl.BlockSpec(
        (addends[0].shape[0], cols * pieces // ways), lambda e, me_ref: (0, side(me_ref))
    )
    piece = (rows, cols // ways)
    return pl.pallas_call(
        functools.partial(pack_body, first, skip, ways, pieces),
        grid_spec=pltpu.PrefetchScalarGridSpec(
            num_scalar_prefetch=1,
            grid=(count // step,),
            in_specs=[SMEM, block, block] + [sums_block] * len(addends),
            out_specs=[pl.BlockSpec((step,) + piece, lambda e, me_ref: (e, 0, 0))] * pieces,
            scratch_shapes=[pltpu.VMEM((pieces,) + piece, jnp.bfloat16)],
        ),
        out_shape=[jax.ShapeDtypeStruct((count,) + piece, jnp.bfloat16)] * pieces,
        name="pack",
    )(me, mix, w, avg, *addends)


def unpack_body(ways, me_ref, *refs):
    out_ref = refs[-1]
    me = me_ref[0]
    step, rows, _ = refs[0].shape
    for k in range(ways):
        at = pl.multiple_of((me ^ k) * rows, rows)
        for i in range(step):
            out_ref[i, pl.ds(at, rows), :] = refs[k][i]


def unpack(me, received, whole, first, total):
    ways = len(received)
    count, rows, width = received[0].shape
    step = step_of(4, count, first)
    held = [] if whole is None else [whole]
    return pl.pallas_call(
        functools.partial(unpack_body, ways),
        grid=(count // step,),
        in_specs=[SMEM]
        + [pl.BlockSpec((step, rows, width), lambda e: (e, 0, 0))] * ways
        + [ANY] * len(held),
        out_specs=pl.BlockSpec((step, ways * rows, width), lambda e: (first // step + e, 0, 0)),
        out_shape=jax.ShapeDtypeStruct((total, ways * rows, width), jnp.bfloat16),
        input_output_aliases={1 + ways: 0} if held else {},
        name="unpack",
    )(me, *received, *held)


def swap(value, k, axis, ways):
    return lax.ppermute(value, axis, [(d, d ^ k) for d in range(ways)])


def crossings(ways):
    return list(reversed(range(ways // 2, ways))) + list(range(1, ways // 2))


def doublings(ways):
    return [1 << b for b in range(ways.bit_length() - 1)]


def router_fold_body(weight_ref, gain_ref, out_ref):
    out_ref[...] = (weight_ref[...] * gain_ref[...]).astype(jnp.bfloat16)


def router_fold(weight, gain):
    full = lambda shape: pl.BlockSpec(shape, lambda: (0, 0))
    return pl.pallas_call(
        router_fold_body,
        in_specs=[full(weight.shape), full(gain.shape)],
        out_specs=full(weight.shape),
        out_shape=jax.ShapeDtypeStruct(weight.shape, jnp.bfloat16),
        name="router_fold",
    )(weight, gain)


def join_body(places, axis, me_ref, in_ref, out_ref):
    size = in_ref.shape[1 + axis]
    for i, place in enumerate(places):
        at = me_ref[0] ^ place
        if out_ref.ndim == 3:
            out_ref[at] = in_ref[i]
        elif axis == 0:
            out_ref[pl.ds(pl.multiple_of(at * size, size), size), :] = in_ref[i]
        else:
            out_ref[:, pl.ds(pl.multiple_of(at * size, size), size)] = in_ref[i]


def join(me, pieces, places, axis):
    shape = list(pieces.shape[1:])
    aligned = axis == 0 or shape[axis] % 128 == 0
    shape[axis] *= len(places)
    made = tuple(shape) if aligned else pieces.shape
    out = pl.pallas_call(
        functools.partial(join_body, places, axis),
        in_specs=[SMEM, pl.BlockSpec(pieces.shape, lambda: (0, 0, 0))],
        out_specs=pl.BlockSpec(made, lambda: (0,) * len(made)),
        out_shape=jax.ShapeDtypeStruct(made, jnp.bfloat16),
        name="join",
    )(me, pieces)
    return out if aligned else jnp.swapaxes(out, 0, 1).reshape(shape)


def gather(value, me, axis, ways, along):
    pieces, places = value[None], [0]
    for k in reversed(doublings(ways)):
        pieces = jnp.concatenate([pieces, swap(pieces, k, axis, ways)], axis=0)
        places = places + [place ^ k for place in places]
    return join(me, pieces, places, along)


def on_device(ways, banks, w_gate, avg_gate, w_up, avg_up, mix_share, router_weight, router_gain):
    experts, rows, cols = w_gate.shape
    width = cols // ways
    index = lax.axis_index("zero")
    me = jnp.reshape(index, (1,))
    my_bank = jnp.reshape(lax.axis_index("bank"), (1,))

    served, scales = [], []
    g = c = 0
    for w, avg, shares in ((w_gate, avg_gate, GATE_GROUPS), (w_up, avg_up, UP_GROUPS)):
        whole, own = None, []
        for chunks in spans(shares, experts):
            start = chunks[0][0]
            members = sum(n for _, n in chunks)
            total = sums(mix_share, w, avg, start, members)
            for k in doublings(ways):
                addends = [total, swap(total, k, "zero", ways)]
                total = addends[0] + addends[1]
            own.append(lax.dynamic_slice_in_dim(total, index * width, width, axis=1))
            for first, count in chunks:
                sent = []
                for part in (0, 1) if g < HALVED and first == start else (None,):
                    sent += pack(
                        me, mix_share, w, avg, addends, first, count, first - start, ways, part
                    )
                received = list(sent)
                for k in crossings(ways):
                    received[k] = swap(sent[k], k, "zero", ways)
                whole = unpack(me, received, whole, first, experts)
                c += 1
            g += 1
        served.append(whole)
        scales.append(jnp.concatenate(own, axis=0) / (ways * rows))

    router = router_fold(router_weight.T, router_gain[None, :])
    router = gather(router, me, "zero", ways, 1)
    router = gather(router, my_bank, "bank", banks, 0)
    return (served[0], served[1], scales[0], scales[1], router.T)


def solution(mesh):
    ways, banks = mesh.shape["zero"], mesh.shape["bank"]
    assert ways & (ways - 1) == 0 and banks & (banks - 1) == 0
    in_specs = (
        P("bank", "zero", None),
        P("bank", "zero", None),
        P("bank", "zero", None),
        P("bank", "zero", None),
        P("bank"),
        P("zero", "bank"),
        P("zero"),
    )
    out_specs = (
        P("bank", None, "zero"),
        P("bank", None, "zero"),
        P("bank", "zero"),
        P("bank", "zero"),
        P(),
    )

    def step(*args):
        def body(*local):
            return on_device(ways, banks, *local)

        local = jax.shard_map(
            body, mesh=mesh, in_specs=in_specs, out_specs=out_specs, check_vma=False
        )
        return local(*args)

    return step
```
